32 devices in a mesh: dp: 4 (over x, core), expert: 4 (over z), etp: 2 (over y).
Axes of the slice: x: 2, y: 2, z: 4, core: 2. Of those that a mesh axis runs over, the one named last changes fastest.
Arguments:
- tokens: bfloat16 [4096, 3072], P(('dp', 'expert'), 'etp'), parts along dimension 0, may hold values from -6 to 6
- experts: int32 [4096, 2], P(('dp', 'expert')), parts along dimension 0, may hold values from 0 to 3, all different within a row; in each aligned block of 256 rows (0 to 255, 256 to 511, ...) at most 176 rows name the same one
- mixing: float32 [4096, 2], P(('dp', 'expert')), parts along dimension 0, may hold values from 0.2 to 1
- up_weight: bfloat16 [4, 3072, 8192], P('expert', None, 'etp'), may hold values from -0.109375 to 0.109375
- down_weight: bfloat16 [4, 8192, 3072], P('expert', 'etp'), may hold values from -0.0625 to 0.0625
Outputs:
- mixed: bfloat16 [4096, 3072], P(('dp', 'expert'), 'etp'), parts along dimension 0
The draws below stay inside these ranges and needn't reach their ends.
There are 4 independent parts, one for each index of `dp`. The reference program is written for one: setup_inputs(seed, part) draws one part's arguments, and reference() takes and returns one part's arrays. A program takes and returns all parts, laid end to end along the dimension named above; an argument that names none is the same for every part. Nothing has to cross between parts.
Inputs may be any that keep to these rules, and one draw needn't show every extreme that they name: Each row names two different experts. In the rows of one index of expert (aligned blocks of 256 rows) no expert is named more than 176 times, a bound that some block reaches.
All inputs are finite; a program needn't handle non-finite values.
Results may differ from the reference program's by a relative error of at most 0.0078.
Values may be sent and summed in bfloat16 or wider, within the bound.
A program may use at most 128 MiB of HBM per device.

```python
import math
import jax
import jax.numpy as jnp
import numpy as np
from jax import lax

D = 3072
FF = 8192
TOK_DEV = 256
E = 4
CAP = 176
TOKENS = 1024


def shard_levels(own_key, shape, pieces, low, high):
    factor_of, own = 1.0, jax.random.fold_in(own_key, 6)
    for position, parts in pieces:
        draws = jnp.exp(jax.random.uniform(jax.random.fold_in(own, position), (parts,), jnp.float32, low / len(pieces), high / len(pieces)))
        factor_of = factor_of * jnp.repeat(draws, shape[position] // parts).reshape([-1 if axis == position else 1 for axis in range(len(shape))])
    return factor_of


def deal_out(stream_key, own, number, rows, amount, top, most, skew):
    ranking = jax.random.permutation(stream_key, amount)
    packed, usual = shares(amount, rows * top, most, skew, True), shares(amount, rows * top, most, skew, False)
    places = jnp.arange(amount)

    def named(lengths, offset_by):
        used = int((lengths > 0).sum())
        fixed = max(1, used // 4)
        moved = fixed + (places - fixed + offset_by * (used - fixed)) % max(1, amount - fixed)
        return jnp.zeros((amount,), jnp.int32).at[ranking[jnp.where(places < fixed, places, moved)]].set(jnp.asarray(lengths, jnp.int32))

    lengths = jnp.where(number % 4 == 0, named(packed, number // 4), named(usual, number - number // 4 - 1))
    mixed = jax.random.permutation(jax.random.fold_in(own, 3), amount)
    giver, sink = mixed[0:amount // 2 * 2:2], mixed[1:amount // 2 * 2:2]
    room = jnp.minimum(lengths[giver] - 1, most - lengths[sink]) // 2
    room = jnp.where((giver == ranking[0]) | (sink == ranking[0]) | (lengths[sink] == 0), 0, jnp.maximum(room, 0))
    moved = jax.random.randint(jax.random.fold_in(own, 4), (amount // 2,), 0, 1 << 20) % (room + 1)
    lengths = lengths.at[giver].add(-moved).at[sink].add(moved)
    members = jnp.searchsorted(jnp.cumsum(lengths), jnp.arange(rows * top), side="right").astype(jnp.int32)
    grid = members.reshape(top, rows).T
    grid = grid[jax.random.permutation(jax.random.fold_in(own, 1), rows)]
    offset_by = jax.random.randint(jax.random.fold_in(own, 2), (rows, 1), 0, top)
    return jnp.take_along_axis(grid, (jnp.arange(top)[None, :] + offset_by) % top, axis=1)


def shares(count, total, reach, skew, full):
    weights = [(1 << 20) // math.isqrt(grade ** skew) + 1 for grade in range(1, count + 1)]
    largest = reach if full else min(reach, max(-(-total // count), total * weights[0] // sum(weights)))
    least = 1 if total - largest >= count - 1 else 0
    holding, spare = [largest] + [least] * (count - 1), total - largest - least * (count - 1)
    while spare > 0:
        candidates = [i for i in range(1, count) if holding[i] < largest] or [i for i in range(1, count) if holding[i] < reach]
        whole, budget = sum([weights[i] for i in candidates]), spare
        for i in candidates:
            extra = min(reach - holding[i], max(1, budget * weights[i] // whole), spare)
            holding[i] = holding[i] + extra
            spare = spare - extra
    return np.array(holding)


def gaussian(key, extent, spread, reach, pieces=(), kind=jnp.bfloat16):
    entries = spread * jax.random.normal(key, extent, jnp.float32)
    if pieces:
        entries = entries * shard_levels(key, extent, pieces, -0.22, 0.18)
    return jnp.clip(entries, -reach, reach).astype(kind)


def setup_inputs(seed: int = 0, part: int = 0) -> dict:
    key_of = jax.random.split(jax.random.key(seed), 6)
    part_splits = jax.random.split(jax.random.fold_in(key_of[5], part), 6)
    tokens = gaussian(part_splits[0], (TOKENS, D), 1.0, 6.0, ((0, 4), (1, 2)))
    experts_keys = jax.random.split(jax.random.fold_in(part_splits[1], 1), TOKENS // TOK_DEV)
    experts_turns = jax.random.permutation(jax.random.fold_in(part_splits[1], 3), TOKENS // TOK_DEV)
    experts = jax.vmap(lambda own, number: deal_out(jax.random.fold_in(part_splits[1], 2), own, number, TOK_DEV, E, 2, CAP, 2))(experts_keys, experts_turns).reshape((TOKENS, 2))
    mixing = jnp.clip(0.2 + 0.8 * jax.random.uniform(part_splits[2], (TOKENS, 2), jnp.float32) ** shard_levels(part_splits[2], (TOKENS, 2), ((0, 4),), -0.2, 0.2), 0.2, 1.0)
    up_weight = gaussian(key_of[3], (E, D, FF), D ** -0.5, 0.109375, ((0, 4), (2, 2)))
    down_weight = gaussian(key_of[4], (E, FF, D), FF ** -0.5, 0.0625, ((0, 4), (1, 2)))
    return dict(tokens=tokens, experts=experts, mixing=mixing, up_weight=up_weight, down_weight=down_weight)


def reference(tokens, experts, mixing, up_weight, down_weight):
    flat_ids = experts.reshape(-1).astype(jnp.int32)
    assigned = flat_ids.shape[0]
    ordering = jnp.arange(assigned, dtype=jnp.int32)
    capacity = CAP * (TOKENS // TOK_DEV)
    flat_mix = mixing.reshape(-1)

    def one_expert(expert):
        sort_key = jnp.where(flat_ids == expert, 0, assigned).astype(jnp.int32) + ordering
        picked = jnp.argsort(sort_key)[:capacity].astype(jnp.int32)
        is_live = flat_ids[picked] == expert
        chosen_rows = tokens[picked // 2]
        up_proj = jnp.dot(chosen_rows, up_weight[expert], preferred_element_type=jnp.float32)
        hidden = jax.nn.silu(up_proj).astype(jnp.bfloat16)
        expert_out = jnp.dot(hidden, down_weight[expert], preferred_element_type=jnp.float32).astype(jnp.bfloat16)
        scaled = jnp.where(is_live, flat_mix[picked], jnp.zeros_like(flat_mix[picked]))
        return expert_out.astype(jnp.float32) * scaled[:, None], picked

    terms, picked = lax.map(one_expert, jnp.arange(E, dtype=jnp.int32))
    mixed = jnp.zeros((TOKENS, D), jnp.float32).at[(picked // 2).reshape(-1)].add(terms.reshape(-1, D))
    return mixed.astype(jnp.bfloat16)
```

```python
import functools

import jax
import jax.numpy as jnp
from jax import lax
from jax.experimental import pallas as pl
from jax.experimental.pallas import tpu as pltpu
from jax.sharding import PartitionSpec as P

MESH = pl.DeviceIdType.MESH
HALVES = 2

TUNED = {
    4: (
        "D0-D1-D3-F00F10",
        "U00V00W00F11F30",
        "U10D2-V10F31W10Y10",
        "U11V11W11F20",
        "U30V30W30Z10Y30",
        "U31V31Y31Z30W31F21F01",
        "U20Y11V20Z31W20Y20",
        "U21V21Y00Z20W21Y21Z11",
        "U01V01W01Z21Y01Z01Z00",
    ),
}


def plan(chunks):
    if chunks in TUNED:
        text = "".join(TUNED[chunks])
        return [
            (text[i], int(text[i + 1]), 0 if text[i + 2] == "-" else int(text[i + 2]))
            for i in range(0, len(text), 3)
        ]
    halves, order = range(HALVES), range(chunks)
    actions = [("D", s, 0) for s in order]
    actions += [("F", s, h) for s in order[:2] for h in halves]
    for s in order:
        actions += [(kind, s, h) for h in halves for kind in "UVYW"]
        actions += [("F", s + 2, h) for h in halves if s + 2 < chunks]
    return actions + [("Z", s, h) for s in reversed(order) for h in halves]


def flipped(index, shift, count):
    total, bit = 0, 1
    while bit < count:
        digit = lax.rem(lax.div(index, bit), 2)
        total = total + (1 - digit if shift & bit else digit) * bit
        bit *= 2
    return total


def layer_kernel(
    chunks, sharers, capacity, actions,
    tok_ref, experts_ref, mixing_ref, up_ref, down_ref, out_ref, share_ref,
    up_v, down_v, full, hidden, other, own, landed, share_v,
    up_sem, down_sem, local_sem,
    zs_sem, zr_sem, ys_sem, yr_sem, bs_sem, br_sem, os_sem, or_sem,
):
    rows, width = tok_ref.shape
    cut, units = hidden.shape
    my_z = lax.axis_index("expert")
    my_y = lax.axis_index("etp")
    z_index = [flipped(my_z, s, chunks) for s in range(chunks)]
    z_peer = [{"expert": z_index[s]} for s in range(chunks)]
    y_index = [flipped(my_y, t, sharers) for t in range(sharers)]
    y_peer = [{"etp": y_index[t]} for t in range(sharers)]
    pieces = [pl.ds(0, cut), pl.ds(cut, capacity - cut)]
    both = range(HALVES)

    def remote(src, dst, send, recv, peer):
        return pltpu.make_async_remote_copy(
            src_ref=src, dst_ref=dst, send_sem=send, recv_sem=recv,
            device_id=peer, device_id_type=MESH,
        )

    def columns(t):
        return pl.ds(t * width, width)

    up_copy, down_copy = [], []
    for t in range(sharers):
        begin = pl.multiple_of(y_index[t] * width, 128)
        up_copy.append(
            pltpu.make_async_copy(
                up_ref.at[pl.ds(begin, width), :], up_v.at[columns(t), :], up_sem.at[t]
            )
        )
        down_copy.append(
            pltpu.make_async_copy(
                down_ref.at[:, pl.ds(begin, width)], down_v.at[:, columns(t)], down_sem.at[t]
            )
        )
    for copy in up_copy + down_copy:
        copy.start()

    barrier = pltpu.get_barrier_semaphore()
    for peer in z_peer[1:] + y_peer[1:]:
        pl.semaphore_signal(barrier, inc=1, device_id=peer, device_id_type=MESH)

    def z_go(s, p):
        return remote(
            own.at[s, pieces[p]], full.at[s, pieces[p], columns(0)],
            zs_sem.at[s, p], zr_sem.at[s, p], z_peer[s],
        )

    def y_go(s, p):
        return [
            remote(
                full.at[s, pieces[p], columns(0)], full.at[s, pieces[p], columns(t)],
                ys_sem.at[s, t, p], yr_sem.at[s, t, p], y_peer[t],
            )
            for t in range(1, sharers)
        ]

    def y_back(s, p):
        return [
            remote(
                other.at[s, t - 1, pieces[p]], landed.at[s, t - 1, pieces[p]],
                bs_sem.at[s, t, p], br_sem.at[s, t, p], y_peer[t],
            )
            for t in range(1, sharers)
        ]

    def z_back(s, p):
        if s == 0:
            return pltpu.make_async_copy(
                own.at[0, pieces[p]], out_ref.at[0, pieces[p]], local_sem.at[p]
            )
        return remote(
            own.at[s, pieces[p]], out_ref.at[s, pieces[p]], os_sem.at[s, p], or_sem.at[s, p],
            z_peer[s],
        )

    share_copy = pltpu.make_async_copy(share_v, share_ref, local_sem.at[HALVES])

    names = experts_ref[...].astype(jnp.float32)
    named = [names[k : k + 1] for k in range(2)]
    mixing = [mixing_ref[k : k + 1, :] for k in range(2)]
    z_name = [z_index[s].astype(jnp.float32) for s in range(chunks)]
    kinds = -(-chunks // 16) * 16
    label = lax.broadcasted_iota(jnp.int32, (kinds, rows), 0).astype(jnp.float32)
    hot = [jnp.where(label == named[k], 1.0, 0.0) for k in range(2)]
    ahead = jnp.where(
        lax.broadcasted_iota(jnp.int32, (rows, rows), 0)
        < lax.broadcasted_iota(jnp.int32, (rows, rows), 1),
        1.0, 0.0,
    ).astype(jnp.bfloat16)
    counts = [
        jnp.dot(hot[k].astype(jnp.bfloat16), ahead, preferred_element_type=jnp.float32)
        for k in range(2)
    ]
    counts[1] = counts[1] + jnp.sum(hot[0], axis=1, keepdims=True)
    place = [jnp.sum(counts[k] * hot[k], axis=0, keepdims=True) for k in range(2)]
    slots = lax.broadcasted_iota(jnp.int32, (capacity, rows), 0).astype(jnp.float32)

    def taken(s, values):
        hit = jnp.zeros((capacity, rows), jnp.float32)
        for k in range(2):
            mine = jnp.where(named[k] == z_name[s], place[k], -1.0)
            hit = hit + jnp.where(slots == mine, values[k], 0.0)
        return hit.astype(jnp.bfloat16)

    greeted = []

    def dispatch(s):
        chunk = jnp.dot(
            taken(s, [1.0, 1.0]), tok_ref[...], preferred_element_type=jnp.float32
        ).astype(jnp.bfloat16)
        if s:
            own[s, pl.ds(0, capacity)] = chunk
        else:
            full[0, pl.ds(0, capacity), columns(0)] = chunk
        if not greeted:
            pl.semaphore_wait(barrier, chunks - 1 + sharers - 1)
            greeted.append(s)
        for p in both:
            for copy in [z_go(s, p)] if s else y_go(0, p):
                copy.start()

    def forward(s, p):
        if s:
            z_go(s, p).wait_recv()
            for copy in y_go(s, p):
                copy.start()

    def finish(s, p):
        for copy in y_back(s, p):
            copy.wait_recv()
        total = own[s, pieces[p]].astype(jnp.float32)
        for t in range(1, sharers):
            total = total + landed[s, t - 1, pieces[p]].astype(jnp.float32)
        own[s, pieces[p]] = total.astype(jnp.bfloat16)
        z_back(s, p).start()

    def send_other(s, p):
        for copy in y_back(s, p):
            copy.start()

    act = {"D": lambda s, p: dispatch(s), "F": forward, "Y": send_other, "Z": finish}

    steps, slot = [], None
    lead = []
    for kind, s, p in actions:
        if kind == "U":
            steps.append(((s, p), [[], [], []]))
            slot = 0
        elif kind in "VW":
            slot = "UVW".index(kind)
        elif not steps:
            lead.append((kind, s, p))
        else:
            steps[-1][1][slot].append((kind, s, p))

    def pick(n, values):
        total = 0
        for k, value in enumerate(values):
            if value:
                total = total + jnp.where(n == k, value, 0)
        return jnp.int32(total)

    for kind, s, p in lead:
        act[kind](s, p)
    share_v[...] = jnp.concatenate([taken(s, mixing) for s in range(chunks)])
    share_copy.start()

    @pl.loop(0, len(steps))
    def _(n):
        chunk = pick(n, [unit[0] for unit, _ in steps])
        at_row = pl.ds(pl.multiple_of(pick(n, [unit[1] * cut for unit, _ in steps]), cut), cut)

        def during(slot):
            for k, (_, slots) in enumerate(steps):
                if slots[slot]:
                    @pl.when(n == k)
                    def _():
                        for kind, s, p in slots[slot]:
                            act[kind](s, p)

        for k, (unit, _) in enumerate(steps):
            @pl.when(n == k)
            def _():
                for copy in y_go(*unit):
                    copy.wait_recv()
                if k == 0:
                    for copy in up_copy:
                        copy.wait()

        tile = 2048 if units % 2048 == 0 else 256

        @pl.loop(0, units // tile)
        def _(i):
            at = pl.ds(pl.multiple_of(i * tile, tile), tile)
            value = jnp.dot(full[chunk, at_row], up_v[:, at], preferred_element_type=jnp.float32)
            hidden[:, at] = (value / (1.0 + jnp.exp(-value))).astype(jnp.bfloat16)

        during(0)

        @pl.when(n == 0)
        def _():
            for copy in down_copy:
                copy.wait()

        for t in range(1, sharers):
            other[chunk, t - 1, at_row] = jnp.dot(
                hidden[...], down_v[:, columns(t)], preferred_element_type=jnp.float32
            ).astype(jnp.bfloat16)
        during(1)
        for k, ((s, p), _) in enumerate(steps):
            if s:
                @pl.when(n == k)
                def _():
                    z_go(s, p).wait_send()
        own[chunk, at_row] = jnp.dot(
            hidden[...], down_v[:, columns(0)], preferred_element_type=jnp.float32
        ).astype(jnp.bfloat16)
        during(2)

    share_copy.wait()
    for s in range(chunks):
        for p in both:
            for copy in y_go(s, p) + y_back(s, p):
                copy.wait_send()
            if s:
                z_back(s, p).wait_send()
                z_back(s, p).wait_recv()
            else:
                z_back(s, p).wait()


def run_layer(tokens, experts, mixing, up_slab, down_slab, chunks, capacity, sharers):
    rows, width = tokens.shape
    model, units = up_slab.shape
    cut = -(-capacity // (16 * HALVES)) * 16
    bf16 = jnp.bfloat16
    dma = pltpu.SemaphoreType.DMA
    anywhere = pl.BlockSpec(memory_space=pl.ANY)
    near = pl.BlockSpec(memory_space=pltpu.VMEM)
    return pl.pallas_call(
        functools.partial(layer_kernel, chunks, sharers, capacity, plan(chunks)),
        out_shape=(
            jax.ShapeDtypeStruct((chunks, capacity, width), bf16),
            jax.ShapeDtypeStruct((chunks * capacity, rows), bf16),
        ),
        in_specs=[near] * 3 + [anywhere] * 2,
        out_specs=(anywhere, anywhere),
        scratch_shapes=[
            pltpu.VMEM((model, units), bf16),
            pltpu.VMEM((units, model), bf16),
            pltpu.VMEM((chunks, HALVES * cut, model), bf16),
            pltpu.VMEM((cut, units), bf16),
            pltpu.VMEM((chunks, sharers - 1, HALVES * cut, width), bf16),
            pltpu.VMEM((chunks, HALVES * cut, width), bf16),
            pltpu.VMEM((chunks, sharers - 1, capacity, width), bf16),
            pltpu.VMEM((chunks * capacity, rows), bf16),
            dma((sharers,)), dma((sharers,)), dma((3,)),
            dma((chunks, 2)), dma((chunks, 2)),
            dma((chunks, sharers, 2)), dma((chunks, sharers, 2)),
            dma((chunks, sharers, 2)), dma((chunks, sharers, 2)),
            dma((chunks, 2)), dma((chunks, 2)),
        ],
        compiler_params=pltpu.CompilerParams(
            collective_id=0, has_side_effects=True, vmem_limit_bytes=67_043_328
        ),
    )(tokens, experts, mixing, up_slab, down_slab)


def local(tokens, experts, mixing, up_weight, down_weight):
    tok_rows, part_width = tokens.shape
    sharers = lax.axis_size("etp")
    expert_count = up_weight.shape[0] * lax.axis_size("expert")
    capacity = 2 * tok_rows // expert_count * 11 // 8
    outputs, share = run_layer(
        tokens, experts.T, mixing.T, up_weight[0], down_weight[0],
        expert_count, capacity, sharers,
    )
    outputs = outputs.reshape(expert_count * capacity, part_width)
    return lax.dot_general(
        share, outputs, (((0,), (0,)), ((), ())), preferred_element_type=jnp.float32
    ).astype(jnp.bfloat16)


def solution(mesh):
    placed = (
        P(("dp", "expert"), "etp"),
        P(("dp", "expert"), None),
        P(("dp", "expert"), None),
        P("expert", None, "etp"),
        P("expert", "etp", None),
    )
    return jax.shard_map(
        local, mesh=mesh, in_specs=placed, out_specs=P(("dp", "expert"), "etp"), check_vma=False
    )
```

```python
import functools

import jax
import jax.numpy as jnp
from jax import lax
from jax.experimental import pallas as pl
from jax.experimental.pallas import tpu as pltpu
from jax.sharding import PartitionSpec as P

MESH = pl.DeviceIdType.MESH
HALVES = 2

TUNED = {
    4: (
        "D0-D1-D3-F10",
        "U00V00W00D2-F30",
        "U10V10F11Y10W10",
        "U30V30F31Y30W30",
        "U11V11Z10W11F20",
        "U31Z30V31Y31W31F21",
        "U20Z31V20Y20W20",
        "U21Y11Z20V21Y21W21Z11Y00",
        "U01V01Z21W01Y01Z01Z00",
    ),
}


def plan(chunks):
    if chunks in TUNED:
        text = "".join(TUNED[chunks])
        return [
            (text[i], int(text[i + 1]), 0 if text[i + 2] == "-" else int(text[i + 2]))
            for i in range(0, len(text), 3)
        ]
    halves, order = range(HALVES), range(chunks)
    actions = [("D", s, 0) for s in order]
    actions += [("F", s, h) for s in order[:2] for h in halves]
    for s in order:
        actions += [(kind, s, h) for h in halves for kind in "UVYW"]
        actions += [("F", s + 2, h) for h in halves if s + 2 < chunks]
    return actions + [("Z", s, h) for s in reversed(order) for h in halves]


def flipped(index, shift, count):
    total, bit = 0, 1
    while bit < count:
        digit = lax.rem(lax.div(index, bit), 2)
        total = total + (1 - digit if shift & bit else digit) * bit
        bit *= 2
    return total


def layer_kernel(
    chunks, sharers, capacity, actions,
    tok_ref, experts_ref, mixing_ref, up_ref, down_ref, out_ref, share_ref,
    up_v, down_v, full, hidden, other, own, landed, share_v,
    up_sem, down_sem, local_sem,
    zs_sem, zr_sem, ys_sem, yr_sem, bs_sem, br_sem, os_sem, or_sem,
):
    rows, width = tok_ref.shape
    units = hidden.shape[1]
    cut = full.shape[1] // HALVES
    my_z = lax.axis_index("expert")
    my_y = lax.axis_index("etp")
    z_index = [flipped(my_z, s, chunks) for s in range(chunks)]
    z_peer = [{"expert": z_index[s]} for s in range(chunks)]
    y_index = [flipped(my_y, t, sharers) for t in range(sharers)]
    y_peer = [{"etp": y_index[t]} for t in range(sharers)]
    pieces = [pl.ds(0, cut), pl.ds(cut, capacity - cut)]
    both = range(HALVES)

    def remote(src, dst, send, recv, peer):
        return pltpu.make_async_remote_copy(
            src_ref=src, dst_ref=dst, send_sem=send, recv_sem=recv,
            device_id=peer, device_id_type=MESH,
        )

    def columns(t):
        return pl.ds(t * width, width)

    up_copy, down_copy = [], []
    for t in range(sharers):
        begin = pl.multiple_of(y_index[t] * width, 128)
        up_copy.append(
            pltpu.make_async_copy(
                up_ref.at[pl.ds(begin, width), :], up_v.at[columns(t), :], up_sem.at[t]
            )
        )
        down_copy.append(
            pltpu.make_async_copy(
                down_ref.at[:, pl.ds(begin, width)], down_v.at[:, columns(t)], down_sem.at[t]
            )
        )
    for copy in up_copy + down_copy:
        copy.start()

    barrier = pltpu.get_barrier_semaphore()
    for peer in z_peer[1:] + y_peer[1:]:
        pl.semaphore_signal(barrier, inc=1, device_id=peer, device_id_type=MESH)

    def z_go(s, p):
        return remote(
            own.at[s, pieces[p]], full.at[s, pieces[p], columns(0)],
            zs_sem.at[s, p], zr_sem.at[s, p], z_peer[s],
        )

    def y_go(s, p):
        return [
            remote(
                full.at[s, pieces[p], columns(0)], full.at[s, pieces[p], columns(t)],
                ys_sem.at[s, t, p], yr_sem.at[s, t, p], y_peer[t],
            )
            for t in range(1, sharers)
        ]

    def y_back(s, p):
        return [
            remote(
                other.at[s, t - 1, pieces[p]], landed.at[s, t - 1, pieces[p]],
                bs_sem.at[s, t, p], br_sem.at[s, t, p], y_peer[t],
            )
            for t in range(1, sharers)
        ]

    def z_back(s, p):
        if s == 0:
            return pltpu.make_async_copy(
                own.at[0, pieces[p]], out_ref.at[0, pieces[p]], local_sem.at[p]
            )
        return remote(
            own.at[s, pieces[p]], out_ref.at[s, pieces[p]], os_sem.at[s, p], or_sem.at[s, p],
            z_peer[s],
        )

    share_copy = pltpu.make_async_copy(share_v, share_ref, local_sem.at[HALVES])

    names = experts_ref[...].astype(jnp.float32)
    named = [names[k : k + 1] for k in range(2)]
    mixing = [mixing_ref[k : k + 1, :] for k in range(2)]
    z_name = [z_index[s].astype(jnp.float32) for s in range(chunks)]
    kinds = -(-chunks // 16) * 16
    label = lax.broadcasted_iota(jnp.int32, (kinds, rows), 0).astype(jnp.float32)
    hot = [jnp.where(label == named[k], 1.0, 0.0) for k in range(2)]
    ahead = jnp.where(
        lax.broadcasted_iota(jnp.int32, (rows, rows), 0)
        < lax.broadcasted_iota(jnp.int32, (rows, rows), 1),
        1.0, 0.0,
    ).astype(jnp.bfloat16)
    counts = [
        jnp.dot(hot[k].astype(jnp.bfloat16), ahead, preferred_element_type=jnp.float32)
        for k in range(2)
    ]
    counts[1] = counts[1] + jnp.sum(hot[0], axis=1, keepdims=True)
    place = [jnp.sum(counts[k] * hot[k], axis=0, keepdims=True) for k in range(2)]
    slots = lax.broadcasted_iota(jnp.int32, (capacity, rows), 0).astype(jnp.float32)

    def taken(s, values):
        hit = jnp.zeros((capacity, rows), jnp.float32)
        for k in range(2):
            mine = jnp.where(named[k] == z_name[s], place[k], -1.0)
            hit = hit + jnp.where(slots == mine, values[k], 0.0)
        return hit.astype(jnp.bfloat16)

    greeted = []

    def dispatch(s):
        chunk = jnp.dot(
            taken(s, [1.0, 1.0]), tok_ref[...], preferred_element_type=jnp.float32
        ).astype(jnp.bfloat16)
        if s:
            own[s, pl.ds(0, capacity)] = chunk
        else:
            full[0, pl.ds(0, capacity), columns(0)] = chunk
        if not greeted:
            pl.semaphore_wait(barrier, chunks - 1 + sharers - 1)
            greeted.append(s)
        for p in both:
            for copy in [z_go(s, p)] if s else y_go(0, p):
                copy.start()

    def forward(s, p):
        if s:
            z_go(s, p).wait_recv()
            for copy in y_go(s, p):
                copy.start()

    def finish(s, p):
        for copy in y_back(s, p):
            copy.wait_recv()
        total = own[s, pieces[p]].astype(jnp.float32)
        for t in range(1, sharers):
            total = total + landed[s, t - 1, pieces[p]].astype(jnp.float32)
        own[s, pieces[p]] = total.astype(jnp.bfloat16)
        z_back(s, p).start()

    def send_other(s, p):
        for copy in y_back(s, p):
            copy.start()

    act = {"D": lambda s, p: dispatch(s), "F": forward, "Y": send_other, "Z": finish}

    steps, slot = [], None
    lead = []
    for kind, s, p in actions:
        if kind == "U":
            steps.append(((s, p), [[], [], []]))
            slot = 0
        elif kind in "VW":
            slot = "UVW".index(kind)
        elif not steps:
            lead.append((kind, s, p))
        else:
            steps[-1][1][slot].append((kind, s, p))

    def pick(n, values):
        total = 0
        for k, value in enumerate(values):
            if value:
                total = total + jnp.where(n == k, value, 0)
        return jnp.int32(total)

    for kind, s, p in lead:
        act[kind](s, p)
    share_v[...] = jnp.concatenate([taken(s, mixing) for s in range(chunks)])
    share_copy.start()

    tile = 2048 if units % 2048 == 0 else 256
    shapes = [(unit[1] == HALVES, unit) for unit, _ in steps]

    @pl.loop(0, len(steps))
    def _(n):
        chunk = pick(n, [unit[0] for _, unit in shapes])
        begin = pick(n, [unit[1] * cut if not big else 0 for big, unit in shapes])
        whole = pick(n, [int(big) for big, _ in shapes]) == 1

        def during(slot):
            for k, (_, slots) in enumerate(steps):
                if slots[slot]:
                    @pl.when(n == k)
                    def _():
                        for kind, s, p in slots[slot]:
                            act[kind](s, p)

        def sized(compute):
            if any(big for big, _ in shapes):
                @pl.when(whole)
                def _():
                    compute(pl.ds(0, capacity), pl.ds(0, capacity))
            if not all(big for big, _ in shapes):
                @pl.when(jnp.logical_not(whole))
                def _():
                    compute(pl.ds(pl.multiple_of(begin, cut), cut), pl.ds(0, cut))

        for k, (big, (s, h)) in enumerate(shapes):
            @pl.when(n == k)
            def _():
                for p in both if big else [h]:
                    for copy in y_go(s, p):
                        copy.wait_recv()
                if k == 0:
                    for copy in up_copy:
                        copy.wait()

        @sized
        def _(at_row, top):
            @pl.loop(0, units // tile)
            def _(i):
                at = pl.ds(pl.multiple_of(i * tile, tile), tile)
                value = jnp.dot(
                    full[chunk, at_row], up_v[:, at], preferred_element_type=jnp.float32
                )
                hidden[top, at] = (value / (1.0 + jnp.exp(-value))).astype(jnp.bfloat16)

        during(0)

        @pl.when(n == 0)
        def _():
            for copy in down_copy:
                copy.wait()

        @sized
        def _(at_row, top):
            for t in range(1, sharers):
                other[chunk, t - 1, at_row] = jnp.dot(
                    hidden[top], down_v[:, columns(t)], preferred_element_type=jnp.float32
                ).astype(jnp.bfloat16)

        during(1)
        for k, (big, (s, h)) in enumerate(shapes):
            if s:
                @pl.when(n == k)
                def _():
                    for p in both if big else [h]:
                        z_go(s, p).wait_send()

        @sized
        def _(at_row, top):
            own[chunk, at_row] = jnp.dot(
                hidden[top], down_v[:, columns(0)], preferred_element_type=jnp.float32
            ).astype(jnp.bfloat16)

        during(2)

    share_copy.wait()
    for s in range(chunks):
        for p in both:
            for copy in y_go(s, p) + y_back(s, p):
                copy.wait_send()
            if s:
                z_back(s, p).wait_send()
                z_back(s, p).wait_recv()
            else:
                z_back(s, p).wait()


def run_layer(tokens, experts, mixing, up_slab, down_slab, chunks, capacity, sharers):
    rows, width = tokens.shape
    model, units = up_slab.shape
    cut = -(-capacity // (16 * HALVES)) * 16
    actions = plan(chunks)
    whole = any(kind == "U" and h == HALVES for kind, _, h in actions)
    most = capacity if whole else cut
    bf16 = jnp.bfloat16
    dma = pltpu.SemaphoreType.DMA
    anywhere = pl.BlockSpec(memory_space=pl.ANY)
    near = pl.BlockSpec(memory_space=pltpu.VMEM)
    return pl.pallas_call(
        functools.partial(layer_kernel, chunks, sharers, capacity, actions),
        out_shape=(
            jax.ShapeDtypeStruct((chunks, capacity, width), bf16),
            jax.ShapeDtypeStruct((chunks * capacity, rows), bf16),
        ),
        in_specs=[near] * 3 + [anywhere] * 2,
        out_specs=(anywhere, anywhere),
        scratch_shapes=[
            pltpu.VMEM((model, units), bf16),
            pltpu.VMEM((units, model), bf16),
            pltpu.VMEM((chunks, HALVES * cut, model), bf16),
            pltpu.VMEM((max(most, cut), units), bf16),
            pltpu.VMEM((chunks, sharers - 1, HALVES * cut, width), bf16),
            pltpu.VMEM((chunks, HALVES * cut, width), bf16),
            pltpu.VMEM((chunks, sharers - 1, capacity, width), bf16),
            pltpu.VMEM((chunks * capacity, rows), bf16),
            dma((sharers,)), dma((sharers,)), dma((3,)),
            dma((chunks, 2)), dma((chunks, 2)),
            dma((chunks, sharers, 2)), dma((chunks, sharers, 2)),
            dma((chunks, sharers, 2)), dma((chunks, sharers, 2)),
            dma((chunks, 2)), dma((chunks, 2)),
        ],
        compiler_params=pltpu.CompilerParams(
            collective_id=0, has_side_effects=True, vmem_limit_bytes=67_043_328
        ),
    )(tokens, experts, mixing, up_slab, down_slab)


def local(tokens, experts, mixing, up_weight, down_weight):
    tok_rows, part_width = tokens.shape
    sharers = lax.axis_size("etp")
    expert_count = up_weight.shape[0] * lax.axis_size("expert")
    capacity = 2 * tok_rows // expert_count * 11 // 8
    outputs, share = run_layer(
        tokens, experts.T, mixing.T, up_weight[0], down_weight[0],
        expert_count, capacity, sharers,
    )
    outputs = outputs.reshape(expert_count * capacity, part_width)
    return lax.dot_general(
        share, outputs, (((0,), (0,)), ((), ())), preferred_element_type=jnp.float32
    ).astype(jnp.bfloat16)


def solution(mesh):
    placed = (
        P(("dp", "expert"), "etp"),
        P(("dp", "expert"), None),
        P(("dp", "expert"), None),
        P("expert", None, "etp"),
        P("expert", "etp", None),
    )
    return jax.shard_map(
        local, mesh=mesh, in_specs=placed, out_specs=P(("dp", "expert"), "etp"), check_vma=False
    )
```

```python
import functools

import jax
import jax.numpy as jnp
from jax import lax
from jax.experimental import pallas as pl
from jax.experimental.pallas import tpu as pltpu
from jax.sharding import PartitionSpec as P

MESH = pl.DeviceIdType.MESH
HALVES = 2

TUNED = {
    4: (
        "D0-D1-D3-F10",
        "U00V00F30W00F11",
        "U10V10D2-F31W10",
        "U30V30Y30W30Y10",
        "U31V31F20Z30W31",
        "U11Z10Y31V11W11F21",
        "U20Z31V20Y20Y11W20",
        "U21V21Z20Y21Y00W21Z11",
        "U01V01Y01Z21Z00W01Z01",
    ),
}


def plan(chunks):
    if chunks in TUNED:
        text = "".join(TUNED[chunks])
        return [
            (text[i], int(text[i + 1]), 0 if text[i + 2] == "-" else int(text[i + 2]))
            for i in range(0, len(text), 3)
        ]
    halves, order = range(HALVES), range(chunks)
    actions = [("D", s, 0) for s in order]
    actions += [("F", s, h) for s in order[:2] for h in halves]
    for s in order:
        actions += [(kind, s, h) for h in halves for kind in "UVYW"]
        actions += [("F", s + 2, h) for h in halves if s + 2 < chunks]
    return actions + [("Z", s, h) for s in reversed(order) for h in halves]


def flipped(index, shift, count):
    total, bit = 0, 1
    while bit < count:
        digit = lax.rem(lax.div(index, bit), 2)
        total = total + (1 - digit if shift & bit else digit) * bit
        bit *= 2
    return total


def layer_kernel(
    chunks, sharers, capacity, actions,
    tok_ref, experts_ref, mixing_ref, up_ref, down_ref, out_ref, share_ref,
    up_v, down_v, full, hidden, other, own, landed, share_v,
    up_sem, down_sem, local_sem,
    zs_sem, zr_sem, ys_sem, yr_sem, bs_sem, br_sem, os_sem, or_sem,
):
    rows, width = tok_ref.shape
    cut, units = hidden.shape
    my_z = lax.axis_index("expert")
    my_y = lax.axis_index("etp")
    z_index = [flipped(my_z, s, chunks) for s in range(chunks)]
    z_peer = [{"expert": z_index[s]} for s in range(chunks)]
    y_index = [flipped(my_y, t, sharers) for t in range(sharers)]
    y_peer = [{"etp": y_index[t]} for t in range(sharers)]
    pieces = [pl.ds(0, cut), pl.ds(cut, capacity - cut)]
    both = range(HALVES)

    def remote(src, dst, send, recv, peer):
        return pltpu.make_async_remote_copy(
            src_ref=src, dst_ref=dst, send_sem=send, recv_sem=recv,
            device_id=peer, device_id_type=MESH,
        )

    def columns(t):
        return pl.ds(t * width, width)

    up_copy, down_copy = [], []
    for t in range(sharers):
        begin = pl.multiple_of(y_index[t] * width, 128)
        up_copy.append(
            pltpu.make_async_copy(
                up_ref.at[pl.ds(begin, width), :], up_v.at[columns(t), :], up_sem.at[t]
            )
        )
        down_copy.append(
            pltpu.make_async_copy(
                down_ref.at[:, pl.ds(begin, width)], down_v.at[:, columns(t)], down_sem.at[t]
            )
        )
    for copy in up_copy + down_copy:
        copy.start()

    barrier = pltpu.get_barrier_semaphore()
    for peer in z_peer[1:] + y_peer[1:]:
        pl.semaphore_signal(barrier, inc=1, device_id=peer, device_id_type=MESH)

    def z_go(s, p):
        return remote(
            own.at[s, pieces[p]], full.at[s, pieces[p], columns(0)],
            zs_sem.at[s, p], zr_sem.at[s, p], z_peer[s],
        )

    def y_go(s, p):
        return [
            remote(
                full.at[s, pieces[p], columns(0)], full.at[s, pieces[p], columns(t)],
                ys_sem.at[s, t, p], yr_sem.at[s, t, p], y_peer[t],
            )
            for t in range(1, sharers)
        ]

    def y_back(s, p):
        return [
            remote(
                other.at[s, t - 1, pieces[p]], landed.at[s, t - 1, pieces[p]],
                bs_sem.at[s, t, p], br_sem.at[s, t, p], y_peer[t],
            )
            for t in range(1, sharers)
        ]

    def z_back(s, p):
        if s == 0:
            return pltpu.make_async_copy(
                own.at[0, pieces[p]], out_ref.at[0, pieces[p]], local_sem.at[p]
            )
        return remote(
            own.at[s, pieces[p]], out_ref.at[s, pieces[p]], os_sem.at[s, p], or_sem.at[s, p],
            z_peer[s],
        )

    share_copy = pltpu.make_async_copy(share_v, share_ref, local_sem.at[HALVES])

    names = experts_ref[...].astype(jnp.float32)
    named = [names[k : k + 1] for k in range(2)]
    mixing = [mixing_ref[k : k + 1, :] for k in range(2)]
    z_name = [z_index[s].astype(jnp.float32) for s in range(chunks)]
    kinds = -(-chunks // 16) * 16
    label = lax.broadcasted_iota(jnp.int32, (kinds, rows), 0).astype(jnp.float32)
    hot = [jnp.where(label == named[k], 1.0, 0.0) for k in range(2)]
    ahead = jnp.where(
        lax.broadcasted_iota(jnp.int32, (rows, rows), 0)
        < lax.broadcasted_iota(jnp.int32, (rows, rows), 1),
        1.0, 0.0,
    ).astype(jnp.bfloat16)
    counts = [
        jnp.dot(hot[k].astype(jnp.bfloat16), ahead, preferred_element_type=jnp.float32)
        for k in range(2)
    ]
    counts[1] = counts[1] + jnp.sum(hot[0], axis=1, keepdims=True)
    place = [jnp.sum(counts[k] * hot[k], axis=0, keepdims=True) for k in range(2)]
    slots = lax.broadcasted_iota(jnp.int32, (capacity, rows), 0).astype(jnp.float32)

    def taken(s, values):
        hit = jnp.zeros((capacity, rows), jnp.float32)
        for k in range(2):
            mine = jnp.where(named[k] == z_name[s], place[k], -1.0)
            hit = hit + jnp.where(slots == mine, values[k], 0.0)
        return hit.astype(jnp.bfloat16)

    greeted = []

    def dispatch(s):
        chunk = jnp.dot(
            taken(s, [1.0, 1.0]), tok_ref[...], preferred_element_type=jnp.float32
        ).astype(jnp.bfloat16)
        if s:
            own[s, pl.ds(0, capacity)] = chunk
        else:
            full[0, pl.ds(0, capacity), columns(0)] = chunk
        if not greeted:
            pl.semaphore_wait(barrier, chunks - 1 + sharers - 1)
            greeted.append(s)
        for p in both:
            for copy in [z_go(s, p)] if s else y_go(0, p):
                copy.start()

    def forward(s, p):
        if s:
            z_go(s, p).wait_recv()
            for copy in y_go(s, p):
                copy.start()

    def finish(s, p):
        for copy in y_back(s, p):
            copy.wait_recv()
        total = own[s, pieces[p]].astype(jnp.float32)
        for t in range(1, sharers):
            total = total + landed[s, t - 1, pieces[p]].astype(jnp.float32)
        own[s, pieces[p]] = total.astype(jnp.bfloat16)
        z_back(s, p).start()

    def send_other(s, p):
        for copy in y_back(s, p):
            copy.start()

    act = {"D": lambda s, p: dispatch(s), "F": forward, "Y": send_other, "Z": finish}

    steps, slot = [], None
    lead = []
    for kind, s, p in actions:
        if kind == "U":
            steps.append(((s, p), [[], [], []]))
            slot = 0
        elif kind in "VW":
            slot = "UVW".index(kind)
        elif not steps:
            lead.append((kind, s, p))
        else:
            steps[-1][1][slot].append((kind, s, p))

    def pick(n, values):
        total = 0
        for k, value in enumerate(values):
            if value:
                total = total + jnp.where(n == k, value, 0)
        return jnp.int32(total)

    for kind, s, p in lead:
        act[kind](s, p)
    share_v[...] = jnp.concatenate([taken(s, mixing) for s in range(chunks)])
    share_copy.start()

    @pl.loop(0, len(steps))
    def _(n):
        chunk = pick(n, [unit[0] for unit, _ in steps])
        at_row = pl.ds(pl.multiple_of(pick(n, [unit[1] * cut for unit, _ in steps]), cut), cut)

        def during(slot):
            for k, (_, slots) in enumerate(steps):
                if slots[slot]:
                    @pl.when(n == k)
                    def _():
                        for kind, s, p in slots[slot]:
                            act[kind](s, p)

        for k, (unit, _) in enumerate(steps):
            @pl.when(n == k)
            def _():
                for copy in y_go(*unit):
                    copy.wait_recv()
                if k == 0:
                    for copy in up_copy:
                        copy.wait()

        tile = 2048 if units % 2048 == 0 else 256

        @pl.loop(0, units // tile)
        def _(i):
            at = pl.ds(pl.multiple_of(i * tile, tile), tile)
            value = jnp.dot(full[chunk, at_row], up_v[:, at], preferred_element_type=jnp.float32)
            hidden[:, at] = (value / (1.0 + jnp.exp(-value))).astype(jnp.bfloat16)

        during(0)

        @pl.when(n == 0)
        def _():
            for copy in down_copy:
                copy.wait()

        for t in range(1, sharers):
            other[chunk, t - 1, at_row] = jnp.dot(
                hidden[...], down_v[:, columns(t)], preferred_element_type=jnp.float32
            ).astype(jnp.bfloat16)
        during(1)
        for k, ((s, p), _) in enumerate(steps):
            if s:
                @pl.when(n == k)
                def _():
                    z_go(s, p).wait_send()
        own[chunk, at_row] = jnp.dot(
            hidden[...], down_v[:, columns(0)], preferred_element_type=jnp.float32
        ).astype(jnp.bfloat16)
        during(2)

    share_copy.wait()
    for s in range(chunks):
        for p in both:
            for copy in y_go(s, p) + y_back(s, p):
                copy.wait_send()
            if s:
                z_back(s, p).wait_send()
                z_back(s, p).wait_recv()
            else:
                z_back(s, p).wait()


def run_layer(tokens, experts, mixing, up_slab, down_slab, chunks, capacity, sharers):
    rows, width = tokens.shape
    model, units = up_slab.shape
    cut = -(-capacity // (16 * HALVES)) * 16
    bf16 = jnp.bfloat16
    dma = pltpu.SemaphoreType.DMA
    anywhere = pl.BlockSpec(memory_space=pl.ANY)
    near = pl.BlockSpec(memory_space=pltpu.VMEM)
    return pl.pallas_call(
        functools.partial(layer_kernel, chunks, sharers, capacity, plan(chunks)),
        out_shape=(
            jax.ShapeDtypeStruct((chunks, capacity, width), bf16),
            jax.ShapeDtypeStruct((chunks * capacity, rows), bf16),
        ),
        in_specs=[near] * 3 + [anywhere] * 2,
        out_specs=(anywhere, anywhere),
        scratch_shapes=[
            pltpu.VMEM((model, units), bf16),
            pltpu.VMEM((units, model), bf16),
            pltpu.VMEM((chunks, HALVES * cut, model), bf16),
            pltpu.VMEM((cut, units), bf16),
            pltpu.VMEM((chunks, sharers - 1, HALVES * cut, width), bf16),
            pltpu.VMEM((chunks, HALVES * cut, width), bf16),
            pltpu.VMEM((chunks, sharers - 1, capacity, width), bf16),
            pltpu.VMEM((chunks * capacity, rows), bf16),
            dma((sharers,)), dma((sharers,)), dma((3,)),
            dma((chunks, 2)), dma((chunks, 2)),
            dma((chunks, sharers, 2)), dma((chunks, sharers, 2)),
            dma((chunks, sharers, 2)), dma((chunks, sharers, 2)),
            dma((chunks, 2)), dma((chunks, 2)),
        ],
        compiler_params=pltpu.CompilerParams(
            collective_id=0, has_side_effects=True, vmem_limit_bytes=67_043_328
        ),
    )(tokens, experts, mixing, up_slab, down_slab)


def local(tokens, experts, mixing, up_weight, down_weight):
    tok_rows, part_width = tokens.shape
    sharers = lax.axis_size("etp")
    expert_count = up_weight.shape[0] * lax.axis_size("expert")
    capacity = 2 * tok_rows // expert_count * 11 // 8
    outputs, share = run_layer(
        tokens, experts.T, mixing.T, up_weight[0], down_weight[0],
        expert_count, capacity, sharers,
    )
    outputs = outputs.reshape(expert_count * capacity, part_width)
    return lax.dot_general(
        share, outputs, (((0,), (0,)), ((), ())), preferred_element_type=jnp.float32
    ).astype(jnp.bfloat16)


def solution(mesh):
    placed = (
        P(("dp", "expert"), "etp"),
        P(("dp", "expert"), None),
        P(("dp", "expert"), None),
        P("expert", None, "etp"),
        P("expert", "etp", None),
    )
    return jax.shard_map(
        local, mesh=mesh, in_specs=placed, out_specs=P(("dp", "expert"), "etp"), check_vma=False
    )
```

```python
import functools

import jax
import jax.numpy as jnp
from jax import lax
from jax.experimental import pallas as pl
from jax.experimental.pallas import tpu as pltpu
from jax.sharding import PartitionSpec as P

MESH = pl.DeviceIdType.MESH
HALVES = 2

TUNED = {
    4: (
        "D0-D1-D3-F10",
        "U00V00F30W00F11",
        "U10V10D2-F31W10",
        "U30V30Y30W30Y10",
        "U31V31F20Z30W31",
        "U11Z10Y31V11W11F21",
        "U20V20Z31Y20Y11W20",
        "U21V21Z20Y21Y00W21Z11",
        "U01V01Y01Z21Z00W01Z01",
    ),
}


def plan(chunks):
    if chunks in TUNED:
        text = "".join(TUNED[chunks])
        return [
            (text[i], int(text[i + 1]), 0 if text[i + 2] == "-" else int(text[i + 2]))
            for i in range(0, len(text), 3)
        ]
    halves, order = range(HALVES), range(chunks)
    actions = [("D", s, 0) for s in order]
    actions += [("F", s, h) for s in order[:2] for h in halves]
    for s in order:
        actions += [(kind, s, h) for h in halves for kind in "UVYW"]
        actions += [("F", s + 2, h) for h in halves if s + 2 < chunks]
    return actions + [("Z", s, h) for s in reversed(order) for h in halves]


def flipped(index, shift, count):
    total, bit = 0, 1
    while bit < count:
        digit = lax.rem(lax.div(index, bit), 2)
        total = total + (1 - digit if shift & bit else digit) * bit
        bit *= 2
    return total


def layer_kernel(
    chunks, sharers, capacity, actions,
    tok_ref, experts_ref, mixing_ref, up_ref, down_ref, out_ref, share_ref,
    up_v, down_v, full, hidden, other, own, landed, share_v,
    up_sem, down_sem, local_sem,
    zs_sem, zr_sem, ys_sem, yr_sem, bs_sem, br_sem, os_sem, or_sem,
):
    rows, width = tok_ref.shape
    cut, units = hidden.shape
    my_z = lax.axis_index("expert")
    my_y = lax.axis_index("etp")
    z_index = [flipped(my_z, s, chunks) for s in range(chunks)]
    z_peer = [{"expert": z_index[s]} for s in range(chunks)]
    y_index = [flipped(my_y, t, sharers) for t in range(sharers)]
    y_peer = [{"etp": y_index[t]} for t in range(sharers)]
    pieces = [pl.ds(0, cut), pl.ds(cut, capacity - cut)]
    both = range(HALVES)

    def remote(src, dst, send, recv, peer):
        return pltpu.make_async_remote_copy(
            src_ref=src, dst_ref=dst, send_sem=send, recv_sem=recv,
            device_id=peer, device_id_type=MESH,
        )

    def columns(t):
        return pl.ds(t * width, width)

    up_copy, down_copy = [], []
    for t in range(sharers):
        begin = pl.multiple_of(y_index[t] * width, 128)
        up_copy.append(
            pltpu.make_async_copy(
                up_ref.at[pl.ds(begin, width), :], up_v.at[columns(t), :], up_sem.at[t]
            )
        )
        down_copy.append(
            pltpu.make_async_copy(
                down_ref.at[:, pl.ds(begin, width)], down_v.at[:, columns(t)], down_sem.at[t]
            )
        )
    for copy in up_copy + down_copy:
        copy.start()

    barrier = pltpu.get_barrier_semaphore()
    for peer in z_peer[1:] + y_peer[1:]:
        pl.semaphore_signal(barrier, inc=1, device_id=peer, device_id_type=MESH)

    def z_go(s, p):
        return remote(
            own.at[s, pieces[p]], full.at[s, pieces[p], columns(0)],
            zs_sem.at[s, p], zr_sem.at[s, p], z_peer[s],
        )

    def y_go(s, p):
        return [
            remote(
                full.at[s, pieces[p], columns(0)], full.at[s, pieces[p], columns(t)],
                ys_sem.at[s, t, p], yr_sem.at[s, t, p], y_peer[t],
            )
            for t in range(1, sharers)
        ]

    def y_back(s, p):
        return [
            remote(
                other.at[s, t - 1, pieces[p]], landed.at[s, t - 1, pieces[p]],
                bs_sem.at[s, t, p], br_sem.at[s, t, p], y_peer[t],
            )
            for t in range(1, sharers)
        ]

    def z_back(s, p):
        if s == 0:
            return pltpu.make_async_copy(
                own.at[0, pieces[p]], out_ref.at[0, pieces[p]], local_sem.at[p]
            )
        return remote(
            own.at[s, pieces[p]], out_ref.at[s, pieces[p]], os_sem.at[s, p], or_sem.at[s, p],
            z_peer[s],
        )

    share_copy = pltpu.make_async_copy(share_v, share_ref, local_sem.at[HALVES])

    names = experts_ref[...].astype(jnp.float32)
    named = [names[k : k + 1] for k in range(2)]
    mixing = [mixing_ref[k : k + 1, :] for k in range(2)]
    z_name = [z_index[s].astype(jnp.float32) for s in range(chunks)]
    kinds = -(-chunks // 16) * 16
    label = lax.broadcasted_iota(jnp.int32, (kinds, rows), 0).astype(jnp.float32)
    hot = [jnp.where(label == named[k], 1.0, 0.0) for k in range(2)]
    ahead = jnp.where(
        lax.broadcasted_iota(jnp.int32, (rows, rows), 0)
        < lax.broadcasted_iota(jnp.int32, (rows, rows), 1),
        1.0, 0.0,
    ).astype(jnp.bfloat16)
    counts = [
        jnp.dot(hot[k].astype(jnp.bfloat16), ahead, preferred_element_type=jnp.float32)
        for k in range(2)
    ]
    counts[1] = counts[1] + jnp.sum(hot[0], axis=1, keepdims=True)
    place = [jnp.sum(counts[k] * hot[k], axis=0, keepdims=True) for k in range(2)]
    slots = lax.broadcasted_iota(jnp.int32, (capacity, rows), 0).astype(jnp.float32)

    def taken(s, values):
        hit = jnp.zeros((capacity, rows), jnp.float32)
        for k in range(2):
            mine = jnp.where(named[k] == z_name[s], place[k], -1.0)
            hit = hit + jnp.where(slots == mine, values[k], 0.0)
        return hit.astype(jnp.bfloat16)

    greeted = []

    def dispatch(s):
        chunk = jnp.dot(
            taken(s, [1.0, 1.0]), tok_ref[...], preferred_element_type=jnp.float32
        ).astype(jnp.bfloat16)
        if s:
            own[s, pl.ds(0, capacity)] = chunk
        else:
            full[0, pl.ds(0, capacity), columns(0)] = chunk
        if not greeted:
            pl.semaphore_wait(barrier, chunks - 1 + sharers - 1)
            greeted.append(s)
        for p in both:
            for copy in [z_go(s, p)] if s else y_go(0, p):
                copy.start()

    def forward(s, p):
        if s:
            z_go(s, p).wait_recv()
            for copy in y_go(s, p):
                copy.start()

    def finish(s, p):
        for copy in y_back(s, p):
            copy.wait_recv()
        total = own[s, pieces[p]].astype(jnp.float32)
        for t in range(1, sharers):
            total = total + landed[s, t - 1, pieces[p]].astype(jnp.float32)
        own[s, pieces[p]] = total.astype(jnp.bfloat16)
        z_back(s, p).start()

    def send_other(s, p):
        for copy in y_back(s, p):
            copy.start()

    act = {"D": lambda s, p: dispatch(s), "F": forward, "Y": send_other, "Z": finish}

    steps, slot = [], None
    lead = []
    for kind, s, p in actions:
        if kind == "U":
            steps.append(((s, p), [[], [], []]))
            slot = 0
        elif kind in "VW":
            slot = "UVW".index(kind)
        elif not steps:
            lead.append((kind, s, p))
        else:
            steps[-1][1][slot].append((kind, s, p))

    def pick(n, values):
        total = 0
        for k, value in enumerate(values):
            if value:
                total = total + jnp.where(n == k, value, 0)
        return jnp.int32(total)

    for kind, s, p in lead:
        act[kind](s, p)
    share_v[...] = jnp.concatenate([taken(s, mixing) for s in range(chunks)])
    share_copy.start()

    @pl.loop(0, len(steps))
    def _(n):
        chunk = pick(n, [unit[0] for unit, _ in steps])
        at_row = pl.ds(pl.multiple_of(pick(n, [unit[1] * cut for unit, _ in steps]), cut), cut)

        def during(slot):
            for k, (_, slots) in enumerate(steps):
                if slots[slot]:
                    @pl.when(n == k)
                    def _():
                        for kind, s, p in slots[slot]:
                            act[kind](s, p)

        for k, (unit, _) in enumerate(steps):
            @pl.when(n == k)
            def _():
                for copy in y_go(*unit):
                    copy.wait_recv()
                if k == 0:
                    for copy in up_copy:
                        copy.wait()

        tile = 2048 if units % 2048 == 0 else 256

        @pl.loop(0, units // tile)
        def _(i):
            at = pl.ds(pl.multiple_of(i * tile, tile), tile)
            value = jnp.dot(full[chunk, at_row], up_v[:, at], preferred_element_type=jnp.float32)
            hidden[:, at] = (value / (1.0 + jnp.exp(-value))).astype(jnp.bfloat16)

        during(0)

        @pl.when(n == 0)
        def _():
            for copy in down_copy:
                copy.wait()

        for t in range(1, sharers):
            other[chunk, t - 1, at_row] = jnp.dot(
                hidden[...], down_v[:, columns(t)], preferred_element_type=jnp.float32
            ).astype(jnp.bfloat16)
        during(1)
        for k, ((s, p), _) in enumerate(steps):
            if s:
                @pl.when(n == k)
                def _():
                    z_go(s, p).wait_send()
        own[chunk, at_row] = jnp.dot(
            hidden[...], down_v[:, columns(0)], preferred_element_type=jnp.float32
        ).astype(jnp.bfloat16)
        during(2)

    share_copy.wait()
    for s in range(chunks):
        for p in both:
            for copy in y_go(s, p) + y_back(s, p):
                copy.wait_send()
            if s:
                z_back(s, p).wait_send()
                z_back(s, p).wait_recv()
            else:
                z_back(s, p).wait()


def run_layer(tokens, experts, mixing, up_slab, down_slab, chunks, capacity, sharers):
    rows, width = tokens.shape
    model, units = up_slab.shape
    cut = -(-capacity // (16 * HALVES)) * 16
    bf16 = jnp.bfloat16
    dma = pltpu.SemaphoreType.DMA
    anywhere = pl.BlockSpec(memory_space=pl.ANY)
    near = pl.BlockSpec(memory_space=pltpu.VMEM)
    return pl.pallas_call(
        functools.partial(layer_kernel, chunks, sharers, capacity, plan(chunks)),
        out_shape=(
            jax.ShapeDtypeStruct((chunks, capacity, width), bf16),
            jax.ShapeDtypeStruct((chunks * capacity, rows), bf16),
        ),
        in_specs=[near] * 3 + [anywhere] * 2,
        out_specs=(anywhere, anywhere),
        scratch_shapes=[
            pltpu.VMEM((model, units), bf16),
            pltpu.VMEM((units, model), bf16),
            pltpu.VMEM((chunks, HALVES * cut, model), bf16),
            pltpu.VMEM((cut, units), bf16),
            pltpu.VMEM((chunks, sharers - 1, HALVES * cut, width), bf16),
            pltpu.VMEM((chunks, HALVES * cut, width), bf16),
            pltpu.VMEM((chunks, sharers - 1, capacity, width), bf16),
            pltpu.VMEM((chunks * capacity, rows), bf16),
            dma((sharers,)), dma((sharers,)), dma((3,)),
            dma((chunks, 2)), dma((chunks, 2)),
            dma((chunks, sharers, 2)), dma((chunks, sharers, 2)),
            dma((chunks, sharers, 2)), dma((chunks, sharers, 2)),
            dma((chunks, 2)), dma((chunks, 2)),
        ],
        compiler_params=pltpu.CompilerParams(
            collective_id=0, has_side_effects=True, vmem_limit_bytes=67_043_328
        ),
    )(tokens, experts, mixing, up_slab, down_slab)


def local(tokens, experts, mixing, up_weight, down_weight):
    tok_rows, part_width = tokens.shape
    sharers = lax.axis_size("etp")
    expert_count = up_weight.shape[0] * lax.axis_size("expert")
    capacity = 2 * tok_rows // expert_count * 11 // 8
    outputs, share = run_layer(
        tokens, experts.T, mixing.T, up_weight[0], down_weight[0],
        expert_count, capacity, sharers,
    )
    outputs = outputs.reshape(expert_count * capacity, part_width)
    return lax.dot_general(
        share, outputs, (((0,), (0,)), ((), ())), preferred_element_type=jnp.float32
    ).astype(jnp.bfloat16)


def solution(mesh):
    placed = (
        P(("dp", "expert"), "etp"),
        P(("dp", "expert"), None),
        P(("dp", "expert"), None),
        P("expert", None, "etp"),
        P("expert", "etp", None),
    )
    return jax.shard_map(
        local, mesh=mesh, in_specs=placed, out_specs=P(("dp", "expert"), "etp"), check_vma=False
    )
```
